32 devices in a mesh: parts: 2 (over y), fsdp: 8 (over z, x), rep: 2 (over core).
Axes of the slice: x: 2, y: 2, z: 4, core: 2. Of those that a mesh axis runs over, the one named last changes fastest.
Arguments:
- tokens: bfloat16 [2, 4096, 5120], P('rep', ('parts', 'fsdp')), parts along dimension 1, may hold values from -6 to 6
- cotangent: bfloat16 [2, 4096, 8], P('rep', ('parts', 'fsdp')), parts along dimension 1, may hold values from -0.1875 to 0.1875
- params: float32 [16, 5120], P(('parts', 'fsdp')), parts along dimension 0, may hold values from -0.078125 to 0.078125
- momentum: float32 [2, 16, 5120], P('rep', ('parts', 'fsdp')), parts along dimension 1, may hold values from -6 to 6
- indices: int32 [2, 16, 40, 16], P('rep', ('parts', 'fsdp')), parts along dimension 1, may hold values from 0 to 127, all different within a row
Outputs:
- new_params: float32 [16, 5120], P(('parts', 'fsdp')), parts along dimension 0
- new_momentum: float32 [2, 16, 5120], P('rep', ('parts', 'fsdp')), parts along dimension 1
The draws below stay inside these ranges and needn't reach their ends.
There are 2 independent parts, one for each index of `parts`. The reference program is written for one: setup_inputs(seed, part) draws one part's arguments, and reference() takes and returns one part's arrays. A program takes and returns all parts, laid end to end along the dimension named above; each array names one. Nothing has to cross between parts.
Inputs may be any that keep to these rules, and one draw needn't show every extreme that they name: Within each block the 16 indices are distinct.
All inputs are finite; a program needn't handle non-finite values.
Results may differ from the reference program's by a relative error of at most 0.0003.
Values sent between devices are 32-bit elements; how exact they have to be, the bound alone decides.
A program may use at most 64 MiB of HBM per device.

```python
import jax
import jax.numpy as jnp
from jax import lax

D = 5120
SPAN = 128
TOPK = 16
ROWS = 8
TOKENS = 2048
NCH = 40
N_REP = 2


def with_spikes(array, stream_key, source, target, blocks, factor):
    owner, partner = [(jnp.arange(array.shape[dim]) // (array.shape[dim] // blocks)).reshape([-1 if axis == dim else 1 for axis in range(array.ndim)]) for dim in (source, target)]
    chosen = jax.random.permutation(stream_key, blocks)[partner]
    strong = (owner == chosen) | (owner == (partner + blocks // 2) % blocks)
    return jnp.where(strong, factor * array, array)


def level_of(stream_key, shape, split, least, high):
    loudness, own = 1.0, jax.random.fold_in(stream_key, 6)
    for dim, shards_of in split:
        steps = jnp.exp(jax.random.uniform(jax.random.fold_in(own, dim), (shards_of,), jnp.float32, least / len(split), high / len(split)))
        loudness = loudness * jnp.repeat(steps, shape[dim] // shards_of).reshape([-1 if axis == dim else 1 for axis in range(len(shape))])
    return loudness


def different_ones(own_key, rows, number_of, top, lift):
    sequence = jax.random.permutation(jax.random.fold_in(own_key, 1), number_of)
    boost = sequence
    for power in range(3):
        boost = boost * boost // number_of
    boost = boost * lift // number_of
    tickets = jax.random.randint(jax.random.fold_in(own_key, 2), (rows, number_of), 0, 4096) + boost
    sure = jax.random.permutation(jax.random.fold_in(own_key, 3), rows)[jnp.arange(number_of) % rows]
    tickets = jnp.where(jnp.arange(rows)[:, None] == sure[None, :], 1 << 14, tickets)
    merit = tickets * number_of + jnp.arange(number_of)
    return lax.top_k(merit.astype(jnp.int32), top)[1].astype(jnp.int32)


def centred(own_key, shape, spread, reach, cuts=(), kind=jnp.bfloat16):
    array = spread * jax.random.normal(own_key, shape, jnp.float32)
    if cuts:
        array = array * level_of(own_key, shape, cuts, -0.22, 0.18)
    return jnp.clip(array, -reach, reach).astype(kind)


def noise_with(rng, extent, spread, bound, cuts, heavy, kind=jnp.bfloat16):
    values = spread * jax.random.normal(rng, extent, jnp.float32)
    if cuts:
        values = values * level_of(rng, extent, cuts, -0.22, 0.18)
    return jnp.clip(with_spikes(values, jax.random.fold_in(rng, 3), *heavy), -bound, bound).astype(kind)


def setup_inputs(seed: int = 0, part: int = 0) -> dict:
    key_of = jax.random.split(jax.random.key(seed), 6)
    part_splits = jax.random.split(jax.random.fold_in(key_of[5], part), 6)
    return {
        "tokens": centred(part_splits[0], (N_REP, TOKENS, D), 1.0, 6.0, ((0, 2), (1, 8))),
        "cotangent": noise_with(part_splits[1], (N_REP, TOKENS, ROWS), (TOKENS ** -0.5), 0.1875, ((0, 2), (1, 8)), (1, 2, 8, 2.0)),
        "params": centred(part_splits[2], (ROWS, D), D ** -0.5, 0.078125, ((0, 8),), jnp.float32),
        "momentum": centred(part_splits[3], (N_REP, ROWS, D), 1.0, 6.0, ((0, 2), (1, 8)), jnp.float32),
        "indices": different_ones(part_splits[4], N_REP * ROWS * NCH, SPAN, TOPK, 0).reshape((N_REP, ROWS, NCH, TOPK)),
    }


momentum_decay = 0.9
learn_rate = 0.5

def span_basis(length):
    freq = jnp.arange(length, dtype=jnp.float32)[:, None]
    place = jnp.arange(length, dtype=jnp.float32)[None, :]
    scale = jnp.where(freq == 0.0, jnp.sqrt(1.0 / length), jnp.sqrt(2.0 / length))
    return (scale * jnp.cos(jnp.pi * (2.0 * place + 1.0) * freq / (2.0 * length))).astype(jnp.float32)

def reference(tokens, cotangent, params, momentum, indices):
    basis = span_basis(SPAN)
    slots = jnp.arange(SPAN, dtype=jnp.int32)
    high = lax.Precision.HIGHEST
    kept_list = []
    sent_list = []
    for group in range(N_REP):
        gradient = lax.dot_general(cotangent[group], tokens[group], (((0,), (0,)), ((), ())), preferred_element_type=jnp.float32)
        moved = momentum_decay * momentum[group] + gradient
        blocks = moved.reshape(ROWS, NCH, SPAN)
        coeffs = jnp.einsum('rjn,kn->rjk', blocks, basis, precision=high)
        selector = (indices[group][..., None] == slots).astype(jnp.float32)
        chosen = jnp.einsum('rjc,rjtc->rjt', coeffs, selector, precision=high)
        sent = jnp.einsum('rjt,rjtc->rjc', chosen, selector, precision=high)
        back = jnp.einsum('rjk,kn->rjn', sent, basis, precision=high).reshape(ROWS, D)
        kept_list.append(moved - back)
        sent_list.append(sent)
    total = sent_list[0]
    for group in range(1, N_REP):
        total = total + sent_list[group]
    mean_sent = total / N_REP
    update = jnp.einsum('rjk,kn->rjn', mean_sent, basis, precision=high).reshape(ROWS, D)
    return (params - learn_rate * update, jnp.stack(kept_list))
```

```python
import functools

import jax
import jax.numpy as jnp
import numpy as np
from jax import lax
from jax.experimental import pallas as pl
from jax.experimental.pallas import tpu as pltpu
from jax.sharding import PartitionSpec as P

MESH = pl.DeviceIdType.MESH

momentum_decay = 0.9
learn_rate = 0.5


def split_basis(length):
    freq = np.arange(length, dtype=np.float64)[:, None]
    place = np.arange(length, dtype=np.float64)[None, :]
    scale = np.where(freq == 0.0, np.sqrt(1.0 / length), np.sqrt(2.0 / length))
    basis = scale * np.cos(np.pi * (2.0 * place + 1.0) * freq / (2.0 * length))

    def stacked(b):
        high = b.astype(jnp.bfloat16)
        low = (b - high.astype(np.float64)).astype(jnp.bfloat16)
        both = np.concatenate([high, low], axis=1)
        return np.concatenate([both, both], axis=0)

    return stacked(basis.T), stacked(basis)


def times(x, w, span):
    high = x.astype(jnp.bfloat16)
    low = (x - high.astype(jnp.float32)).astype(jnp.bfloat16)
    out = jnp.dot(
        jnp.concatenate([high, low], axis=1), w, preferred_element_type=jnp.float32
    )
    return out[:, :span] + out[:, span:]


def kernel(
    n, reps, tok_hbm, cot_hbm, par_hbm, mom_hbm, idx_hbm, wf_hbm, wb_hbm,
    newp_hbm, newm_hbm,
    tok, cot, par, mom, idx, wf, wb, newp, newm, send, recv, back, peer, mask,
    tok_sem, in_sem, out_sem, send_sem, recv_sem, bsend_sem, brecv_sem,
):
    me = lax.axis_index("fsdp")
    my_rep = lax.axis_index("rep")
    chunks, _, rows_dev, cb, span = send.shape
    rows = n * rows_dev
    cols = cb * span

    barrier = pltpu.get_barrier_semaphore()

    def greet(d):
        pl.semaphore_signal(
            barrier, inc=1, device_id={"fsdp": lax.rem(me + d, n)}, device_id_type=MESH
        )

    def over_peers(body):
        if n <= 16:
            for d in range(n - 1, 0, -1):
                body(d)
        else:
            lax.fori_loop(1, n, lambda d, c: (body(d), c)[1], 0)

    small = [(cot_hbm, cot), (par_hbm, par), (mom_hbm, mom), (idx_hbm, idx), (wf_hbm, wf), (wb_hbm, wb)]
    in_copies = [
        pltpu.make_async_copy(src, dst, in_sem.at[i]) for i, (src, dst) in enumerate(small)
    ]
    tok_copies = [
        pltpu.make_async_copy(
            tok_hbm.at[:, pl.ds(c * cols, cols)], tok.at[c], tok_sem.at[c]
        )
        for c in range(chunks)
    ]
    over_peers(greet)
    for a in range(1, reps):
        pl.semaphore_signal(
            barrier, inc=1, device_id={"rep": lax.rem(my_rep + a, reps)}, device_id_type=MESH
        )
    in_copies[0].start()
    for c in range(chunks):
        tok_copies[c].start()
    for i in range(1, len(small)):
        in_copies[i].start()

    in_copies[0].wait()
    lhs = cot[...]
    for c in range(chunks):
        tok_copies[c].wait()
        part = jnp.dot(lhs, tok[c], preferred_element_type=jnp.float32)
        for j in range(cb):
            send[c, :, :, j, :] = part[:, j * span : (j + 1) * span].reshape(n, rows_dev, span)
        if c == 0:
            pl.semaphore_wait(barrier, n - 1 + reps - 1)

        def scatter(d, c=c):
            to = lax.rem(me + d, n)
            pltpu.make_async_remote_copy(
                src_ref=send.at[c, to],
                dst_ref=recv.at[c, d - 1],
                send_sem=send_sem.at[c],
                recv_sem=recv_sem.at[c],
                device_id={"fsdp": to},
                device_id_type=MESH,
            ).start()

        over_peers(scatter)

    for i in range(1, len(small)):
        in_copies[i].wait()
    slots = lax.broadcasted_iota(jnp.int32, (cb, span), 1)
    for r in range(rows_dev):
        turned = idx[r].T
        for c in range(chunks):
            picks = turned[c * cb : (c + 1) * cb, :]
            hit = picks[:, 0:1] == slots
            for t in range(1, picks.shape[1]):
                hit = jnp.logical_or(hit, picks[:, t : t + 1] == slots)
            mask[c, r * cb : (r + 1) * cb, :] = hit.astype(jnp.float32)

    def scattered(c):
        return pltpu.make_async_remote_copy(
            src_ref=send.at[c, pl.ds(0, n - 1)],
            dst_ref=recv.at[c, pl.ds(0, n - 1)],
            send_sem=send_sem.at[c],
            recv_sem=recv_sem.at[c],
            device_id={"fsdp": lax.rem(me + 1, n)},
            device_id_type=MESH,
        )

    def swap(c, a):
        return pltpu.make_async_remote_copy(
            src_ref=back.at[c],
            dst_ref=peer.at[a - 1, c],
            send_sem=bsend_sem.at[a - 1, c],
            recv_sem=brecv_sem.at[a - 1, c],
            device_id={"rep": lax.rem(my_rep + a, reps)},
            device_id_type=MESH,
        )

    for c in range(chunks):
        blocks = pl.ds(c * cb, cb)
        mine = send[c, me] + momentum_decay * mom[:, blocks, :]
        scattered(c).wait_recv()
        moved = mine + jnp.sum(recv[c], axis=0)
        moved = moved.reshape(rows_dev * cb, span)
        coeffs = times(moved, wf[...], span)
        sent = coeffs * mask[c]
        undone = times(sent, wb[...], span)
        back[c] = undone
        for a in range(1, reps):
            swap(c, a).start()
        newm[:, blocks, :] = (moved - undone).reshape(rows_dev, cb, span)
    newm_copy = pltpu.make_async_copy(newm, newm_hbm, out_sem.at[0])
    newm_copy.start()
    for c in range(chunks):
        blocks = pl.ds(c * cb, cb)
        total = back[c]
        for a in range(1, reps):
            swap(c, a).wait_recv()
            total = total + peer[a - 1, c]
        newp[:, blocks, :] = par[:, blocks, :] - (learn_rate / reps) * total.reshape(
            rows_dev, cb, span
        )
    newp_copy = pltpu.make_async_copy(newp, newp_hbm, out_sem.at[1])
    newp_copy.start()
    for c in range(chunks):
        scattered(c).wait_send()
        for a in range(1, reps):
            swap(c, a).wait_send()
    newm_copy.wait()
    newp_copy.wait()


def local(n, reps, tokens, cotangent, params, momentum, indices):
    _, count, width = tokens.shape
    rows_dev, blocks_row, topk = indices.shape[1:]
    span = width // blocks_row
    cb = 8 if blocks_row % 8 == 0 else blocks_row
    chunks = blocks_row // cb
    rows = cotangent.shape[2]
    wf, wb = split_basis(span)
    shape = (rows_dev, blocks_row, span)
    f32 = jnp.float32
    anywhere = pl.BlockSpec(memory_space=pl.ANY)
    newp, newm = pl.pallas_call(
        functools.partial(kernel, n, reps),
        out_shape=[jax.ShapeDtypeStruct(shape, f32)] * 2,
        in_specs=[anywhere] * 7,
        out_specs=[anywhere] * 2,
        scratch_shapes=[
            pltpu.VMEM((chunks, count, cb * span), tokens.dtype),
            pltpu.VMEM((rows, count), cotangent.dtype),
            pltpu.VMEM(shape, f32),
            pltpu.VMEM(shape, f32),
            pltpu.VMEM((rows_dev, topk, blocks_row), indices.dtype),
            pltpu.VMEM(wf.shape, jnp.bfloat16),
            pltpu.VMEM(wb.shape, jnp.bfloat16),
            pltpu.VMEM(shape, f32),
            pltpu.VMEM(shape, f32),
            pltpu.VMEM((chunks, n, rows_dev, cb, span), f32),
            pltpu.VMEM((chunks, n - 1, rows_dev, cb, span), f32),
            pltpu.VMEM((chunks, rows_dev * cb, span), f32),
            pltpu.VMEM((reps - 1, chunks, rows_dev * cb, span), f32),
            pltpu.VMEM((chunks, rows_dev * cb, span), f32),
            pltpu.SemaphoreType.DMA((chunks,)),
            pltpu.SemaphoreType.DMA((6,)),
            pltpu.SemaphoreType.DMA((2,)),
            pltpu.SemaphoreType.DMA((chunks,)),
            pltpu.SemaphoreType.DMA((chunks,)),
            pltpu.SemaphoreType.DMA((reps - 1, chunks)),
            pltpu.SemaphoreType.DMA((reps - 1, chunks)),
        ],
        compiler_params=pltpu.CompilerParams(collective_id=0, has_side_effects=True),
    )(
        tokens[0],
        cotangent[0].T,
        params.reshape(shape),
        momentum.reshape(shape),
        indices[0].transpose(0, 2, 1),
        jnp.asarray(wf),
        jnp.asarray(wb),
    )
    return newp.reshape(rows_dev, width), newm.reshape(1, rows_dev, width)


def solution(mesh):
    in_specs = (
        P("rep", ("parts", "fsdp"), None),
        P("rep", ("parts", "fsdp"), None),
        P(("parts", "fsdp"), None),
        P("rep", ("parts", "fsdp"), None),
        P("rep", ("parts", "fsdp"), None, None),
    )
    out_specs = (P(("parts", "fsdp"), None), P("rep", ("parts", "fsdp"), None))
    body = functools.partial(local, mesh.shape["fsdp"], mesh.shape["rep"])
    return jax.shard_map(body, mesh=mesh, in_specs=in_specs, out_specs=out_specs, check_vma=False)
```

```python
import functools

import jax
import jax.numpy as jnp
import numpy as np
from jax import lax
from jax.experimental import pallas as pl
from jax.experimental.pallas import tpu as pltpu
from jax.sharding import PartitionSpec as P

MESH = pl.DeviceIdType.MESH

momentum_decay = 0.9
learn_rate = 0.5


def split_basis(length):
    freq = np.arange(length, dtype=np.float64)[:, None]
    place = np.arange(length, dtype=np.float64)[None, :]
    scale = np.where(freq == 0.0, np.sqrt(1.0 / length), np.sqrt(2.0 / length))
    basis = scale * np.cos(np.pi * (2.0 * place + 1.0) * freq / (2.0 * length))

    def stacked(b):
        high = b.astype(jnp.bfloat16)
        low = (b - high.astype(np.float64)).astype(jnp.bfloat16)
        both = np.concatenate([high, low], axis=1)
        return np.concatenate([both, both], axis=0)

    return stacked(basis.T), stacked(basis)


def times(x, w, span):
    high = x.astype(jnp.bfloat16)
    low = (x - high.astype(jnp.float32)).astype(jnp.bfloat16)
    out = jnp.dot(
        jnp.concatenate([high, low], axis=1), w, preferred_element_type=jnp.float32
    )
    return out[:, :span] + out[:, span:]


def kernel(
    n, reps, tok_hbm, cot_hbm, par_hbm, mom_hbm, idx_hbm, wf_hbm, wb_hbm,
    newp, newm,
    tok, cot, par, mom, idx, wf, wb, send, recv, back, peer, mask,
    tok_sem, in_sem, send_sem, recv_sem, bsend_sem, brecv_sem,
):
    me = lax.axis_index("fsdp")
    my_rep = lax.axis_index("rep")
    chunks, _, rows_dev, cb, span = send.shape
    rows = n * rows_dev
    cols = cb * span

    barrier = pltpu.get_barrier_semaphore()

    def greet(d):
        pl.semaphore_signal(
            barrier, inc=1, device_id={"fsdp": lax.rem(me + d, n)}, device_id_type=MESH
        )

    def over_peers(body):
        if n <= 16:
            for d in range(n - 1, 0, -1):
                body(d)
        else:
            lax.fori_loop(1, n, lambda d, c: (body(d), c)[1], 0)

    small = [(cot_hbm, cot), (par_hbm, par), (mom_hbm, mom), (idx_hbm, idx), (wf_hbm, wf), (wb_hbm, wb)]
    in_copies = [
        pltpu.make_async_copy(src, dst, in_sem.at[i]) for i, (src, dst) in enumerate(small)
    ]
    tok_copies = [
        pltpu.make_async_copy(
            tok_hbm.at[:, pl.ds(c * cols, cols)], tok.at[c], tok_sem.at[c]
        )
        for c in range(chunks)
    ]
    over_peers(greet)
    for a in range(1, reps):
        pl.semaphore_signal(
            barrier, inc=1, device_id={"rep": lax.rem(my_rep + a, reps)}, device_id_type=MESH
        )
    in_copies[0].start()
    for c in range(chunks):
        tok_copies[c].start()
    for i in range(1, len(small)):
        in_copies[i].start()

    in_copies[0].wait()
    lhs = cot[...]
    for c in range(chunks):
        tok_copies[c].wait()
        part = jnp.dot(lhs, tok[c], preferred_element_type=jnp.float32)
        for j in range(cb):
            send[c, :, :, j, :] = part[:, j * span : (j + 1) * span].reshape(n, rows_dev, span)
        if c == 0:
            pl.semaphore_wait(barrier, n - 1 + reps - 1)

        def scatter(d, c=c):
            to = lax.rem(me + d, n)
            pltpu.make_async_remote_copy(
                src_ref=send.at[c, to],
                dst_ref=recv.at[c, d - 1],
                send_sem=send_sem.at[c],
                recv_sem=recv_sem.at[c],
                device_id={"fsdp": to},
                device_id_type=MESH,
            ).start()

        over_peers(scatter)

    for i in range(1, len(small)):
        in_copies[i].wait()
    slots = lax.broadcasted_iota(jnp.int32, (cb, span), 1)
    for r in range(rows_dev):
        turned = idx[r].T
        for c in range(chunks):
            picks = turned[c * cb : (c + 1) * cb, :]
            hit = picks[:, 0:1] == slots
            for t in range(1, picks.shape[1]):
                hit = jnp.logical_or(hit, picks[:, t : t + 1] == slots)
            mask[c, r * cb : (r + 1) * cb, :] = hit.astype(jnp.float32)

    def scattered(c):
        return pltpu.make_async_remote_copy(
            src_ref=send.at[c, pl.ds(0, n - 1)],
            dst_ref=recv.at[c, pl.ds(0, n - 1)],
            send_sem=send_sem.at[c],
            recv_sem=recv_sem.at[c],
            device_id={"fsdp": lax.rem(me + 1, n)},
            device_id_type=MESH,
        )

    def swap(c, a):
        return pltpu.make_async_remote_copy(
            src_ref=back.at[c],
            dst_ref=peer.at[a - 1, c],
            send_sem=bsend_sem.at[a - 1, c],
            recv_sem=brecv_sem.at[a - 1, c],
            device_id={"rep": lax.rem(my_rep + a, reps)},
            device_id_type=MESH,
        )

    for c in range(chunks):
        blocks = pl.ds(c * cb, cb)
        mine = send[c, me] + momentum_decay * mom[:, blocks, :]
        scattered(c).wait_recv()
        moved = mine + jnp.sum(recv[c], axis=0)
        moved = moved.reshape(rows_dev * cb, span)
        coeffs = times(moved, wf[...], span)
        sent = coeffs * mask[c]
        undone = times(sent, wb[...], span)
        back[c] = undone
        for a in range(1, reps):
            swap(c, a).start()
        newm[:, blocks, :] = (moved - undone).reshape(rows_dev, cb, span)
    for c in range(chunks):
        blocks = pl.ds(c * cb, cb)
        total = back[c]
        for a in range(1, reps):
            swap(c, a).wait_recv()
            total = total + peer[a - 1, c]
        newp[:, blocks, :] = par[:, blocks, :] - (learn_rate / reps) * total.reshape(
            rows_dev, cb, span
        )
    for c in range(chunks):
        scattered(c).wait_send()
        for a in range(1, reps):
            swap(c, a).wait_send()


def put(newp, newm, newp_hbm, newm_hbm, out_sem):
    copies = [
        pltpu.make_async_copy(newp, newp_hbm, out_sem.at[0]),
        pltpu.make_async_copy(newm, newm_hbm, out_sem.at[1]),
    ]
    for copy in copies:
        copy.start()
    for copy in copies:
        copy.wait()


def local(n, reps, tokens, cotangent, params, momentum, indices):
    _, count, width = tokens.shape
    rows_dev, blocks_row, topk = indices.shape[1:]
    span = width // blocks_row
    cb = 8 if blocks_row % 8 == 0 else blocks_row
    chunks = blocks_row // cb
    rows = cotangent.shape[2]
    wf, wb = split_basis(span)
    shape = (rows_dev, blocks_row, span)
    f32 = jnp.float32
    remote = pl.BlockSpec(memory_space=pltpu.HBM)
    near = pl.BlockSpec(memory_space=pltpu.VMEM)
    operands = (
        tokens[0],
        cotangent[0].T,
        params.reshape(shape),
        momentum.reshape(shape),
        indices[0].transpose(0, 2, 1),
        jnp.asarray(wf),
        jnp.asarray(wb),
    )
    newp, newm = pl.pallas_call(
        functools.partial(kernel, n, reps),
        out_shape=[jax.ShapeDtypeStruct(shape, f32)] * 2,
        in_specs=[remote] * len(operands),
        out_specs=[near] * 2,
        scratch_shapes=[
            pltpu.VMEM((chunks, count, cb * span), tokens.dtype),
            pltpu.VMEM((rows, count), cotangent.dtype),
            pltpu.VMEM(shape, f32),
            pltpu.VMEM(shape, f32),
            pltpu.VMEM((rows_dev, topk, blocks_row), indices.dtype),
            pltpu.VMEM(wf.shape, jnp.bfloat16),
            pltpu.VMEM(wb.shape, jnp.bfloat16),
            pltpu.VMEM((chunks, n, rows_dev, cb, span), f32),
            pltpu.VMEM((chunks, n - 1, rows_dev, cb, span), f32),
            pltpu.VMEM((chunks, rows_dev * cb, span), f32),
            pltpu.VMEM((reps - 1, chunks, rows_dev * cb, span), f32),
            pltpu.VMEM((chunks, rows_dev * cb, span), f32),
            pltpu.SemaphoreType.DMA((chunks,)),
            pltpu.SemaphoreType.DMA((6,)),
            pltpu.SemaphoreType.DMA((chunks,)),
            pltpu.SemaphoreType.DMA((chunks,)),
            pltpu.SemaphoreType.DMA((reps - 1, chunks)),
            pltpu.SemaphoreType.DMA((reps - 1, chunks)),
        ],
        compiler_params=pltpu.CompilerParams(
            collective_id=0, has_side_effects=True, vmem_limit_bytes=24 << 20
        ),
    )(*(pltpu.with_memory_space_constraint(x, pltpu.HBM) for x in operands))
    newp, newm = pl.pallas_call(
        put,
        out_shape=[jax.ShapeDtypeStruct(shape, f32)] * 2,
        in_specs=[near] * 2,
        out_specs=[remote] * 2,
        scratch_shapes=[pltpu.SemaphoreType.DMA((2,))],
        compiler_params=pltpu.CompilerParams(vmem_limit_bytes=1 << 20),
    )(newp, newm)
    return newp.reshape(rows_dev, width), newm.reshape(1, rows_dev, width)


def solution(mesh):
    in_specs = (
        P("rep", ("parts", "fsdp"), None),
        P("rep", ("parts", "fsdp"), None),
        P(("parts", "fsdp"), None),
        P("rep", ("parts", "fsdp"), None),
        P("rep", ("parts", "fsdp"), None, None),
    )
    out_specs = (P(("parts", "fsdp"), None), P("rep", ("parts", "fsdp"), None))
    body = functools.partial(local, mesh.shape["fsdp"], mesh.shape["rep"])
    return jax.shard_map(body, mesh=mesh, in_specs=in_specs, out_specs=out_specs, check_vma=False)
```

```python
import functools

import jax
import jax.numpy as jnp
import numpy as np
from jax import lax
from jax.experimental import pallas as pl
from jax.experimental.pallas import tpu as pltpu
from jax.sharding import PartitionSpec as P

MESH = pl.DeviceIdType.MESH

momentum_decay = 0.9
learn_rate = 0.5


def split_basis(length):
    freq = np.arange(length, dtype=np.float64)[:, None]
    place = np.arange(length, dtype=np.float64)[None, :]
    scale = np.where(freq == 0.0, np.sqrt(1.0 / length), np.sqrt(2.0 / length))
    basis = scale * np.cos(np.pi * (2.0 * place + 1.0) * freq / (2.0 * length))

    def stacked(b):
        high = b.astype(jnp.bfloat16)
        low = (b - high.astype(np.float64)).astype(jnp.bfloat16)
        both = np.concatenate([high, low], axis=1)
        return np.concatenate([both, both], axis=0)

    return stacked(basis.T), stacked(basis)


def times(x, w, span):
    high = x.astype(jnp.bfloat16)
    low = (x - high.astype(jnp.float32)).astype(jnp.bfloat16)
    out = jnp.dot(
        jnp.concatenate([high, low], axis=1), w, preferred_element_type=jnp.float32
    )
    return out[:, :span] + out[:, span:]


def kernel(
    n, reps, tok_hbm, cot_hbm, par_hbm, mom_hbm, idx_hbm, wf_hbm, wb_hbm,
    newp, newm,
    tok, cot, par, mom, idx, wf, wb, send, recv, back, peer, mask,
    tok_sem, in_sem, send_sem, recv_sem, bsend_sem, brecv_sem,
):
    me = lax.axis_index("fsdp")
    my_rep = lax.axis_index("rep")
    chunks, _, rows_dev, cb, span = send.shape
    rows = n * rows_dev
    cols = cb * span

    barrier = pltpu.get_barrier_semaphore()

    def greet(d):
        pl.semaphore_signal(
            barrier, inc=1, device_id={"fsdp": lax.rem(me + d, n)}, device_id_type=MESH
        )

    def over_peers(body, first=1, last=n):
        if n <= 16:
            for d in range(first, last):
                body(d)
        else:
            lax.fori_loop(first, last, lambda d, c: (body(d), c)[1], 0)

    small = [(cot_hbm, cot), (par_hbm, par), (mom_hbm, mom), (idx_hbm, idx), (wf_hbm, wf), (wb_hbm, wb)]
    in_copies = [
        pltpu.make_async_copy(src, dst, in_sem.at[i]) for i, (src, dst) in enumerate(small)
    ]
    tok_copies = [
        pltpu.make_async_copy(
            tok_hbm.at[:, pl.ds(c * cols, cols)], tok.at[c], tok_sem.at[c]
        )
        for c in range(chunks)
    ]
    over_peers(greet)
    for a in range(1, reps):
        pl.semaphore_signal(
            barrier, inc=1, device_id={"rep": lax.rem(my_rep + a, reps)}, device_id_type=MESH
        )
    in_copies[0].start()
    for c in range(chunks):
        tok_copies[c].start()
    for i in range(1, len(small)):
        in_copies[i].start()

    def scatter(d, c):
        past = (d - 1 + n - me) // n
        to = d - 1 + past
        pltpu.make_async_remote_copy(
            src_ref=send.at[c, to],
            dst_ref=recv.at[c, me - 1 + past],
            send_sem=send_sem.at[c],
            recv_sem=recv_sem.at[c],
            device_id={"fsdp": to},
            device_id_type=MESH,
        ).start()

    early = min(1, n - 1)
    in_copies[0].wait()
    lhs = cot[...]
    for c in range(chunks):
        tok_copies[c].wait()
        part = jnp.dot(lhs, tok[c], preferred_element_type=jnp.float32)
        for j in range(cb):
            send[c, :, :, j, :] = part[:, j * span : (j + 1) * span].reshape(n, rows_dev, span)
        if c == 0:
            pl.semaphore_wait(barrier, n - 1 + reps - 1)

        over_peers(functools.partial(scatter, c=c), 1, 1 + early)
    for c in range(chunks):
        over_peers(functools.partial(scatter, c=c), 1 + early, n)

    for i in range(1, len(small)):
        in_copies[i].wait()
    slots = lax.broadcasted_iota(jnp.int32, (cb, span), 1)
    for r in range(rows_dev):
        turned = idx[r].T
        for c in range(chunks):
            picks = turned[c * cb : (c + 1) * cb, :]
            hit = picks[:, 0:1] == slots
            for t in range(1, picks.shape[1]):
                hit = jnp.logical_or(hit, picks[:, t : t + 1] == slots)
            mask[(c * rows_dev + r) * cb : (c * rows_dev + r + 1) * cb, :] = hit.astype(jnp.float32)

    def scattered(c):
        return pltpu.make_async_remote_copy(
            src_ref=send.at[c, pl.ds(0, n - 1)],
            dst_ref=recv.at[c, pl.ds(0, n - 1)],
            send_sem=send_sem.at[c],
            recv_sem=recv_sem.at[c],
            device_id={"fsdp": lax.rem(me + 1, n)},
            device_id_type=MESH,
        )

    def swap(a):
        return pltpu.make_async_remote_copy(
            src_ref=back,
            dst_ref=peer.at[a - 1],
            send_sem=bsend_sem.at[a - 1],
            recv_sem=brecv_sem.at[a - 1],
            device_id={"rep": lax.rem(my_rep + a, reps)},
            device_id_type=MESH,
        )

    parts = []
    for c in range(chunks):
        mine = send[c, me] + momentum_decay * mom[:, pl.ds(c * cb, cb), :]
        scattered(c).wait_recv()
        parts.append((mine + jnp.sum(recv[c], axis=0)).reshape(rows_dev * cb, span))
    moved = jnp.concatenate(parts, axis=0)
    sent = times(moved, wf[...], span) * mask[...]
    undone = times(sent, wb[...], span)
    back[...] = undone
    for a in range(1, reps):
        swap(a).start()
    kept = moved - undone
    size = rows_dev * cb
    for c in range(chunks):
        newm[:, pl.ds(c * cb, cb), :] = kept[c * size : (c + 1) * size].reshape(rows_dev, cb, span)
        scattered(c).wait_send()
    for a in range(1, reps):
        swap(a).wait_recv()
        undone = undone + peer[a - 1]
    for c in range(chunks):
        blocks = pl.ds(c * cb, cb)
        newp[:, blocks, :] = par[:, blocks, :] - (learn_rate / reps) * undone[
            c * size : (c + 1) * size
        ].reshape(rows_dev, cb, span)
    for a in range(1, reps):
        swap(a).wait_send()


def put(newp, newm, newp_hbm, newm_hbm, out_sem):
    copies = [
        pltpu.make_async_copy(newp, newp_hbm, out_sem.at[0]),
        pltpu.make_async_copy(newm, newm_hbm, out_sem.at[1]),
    ]
    for copy in copies:
        copy.start()
    for copy in copies:
        copy.wait()


def local(n, reps, tokens, cotangent, params, momentum, indices):
    _, count, width = tokens.shape
    rows_dev, blocks_row, topk = indices.shape[1:]
    span = width // blocks_row
    cb = 8 if blocks_row % 8 == 0 else blocks_row
    chunks = blocks_row // cb
    rows = cotangent.shape[2]
    wf, wb = split_basis(span)
    shape = (rows_dev, blocks_row, span)
    f32 = jnp.float32
    remote = pl.BlockSpec(memory_space=pltpu.HBM)
    near = pl.BlockSpec(memory_space=pltpu.VMEM)
    operands = (
        tokens[0],
        cotangent[0].T,
        params.reshape(shape),
        momentum.reshape(shape),
        indices[0].transpose(0, 2, 1),
        jnp.asarray(wf),
        jnp.asarray(wb),
    )
    newp, newm = pl.pallas_call(
        functools.partial(kernel, n, reps),
        out_shape=[jax.ShapeDtypeStruct(shape, f32)] * 2,
        in_specs=[remote] * len(operands),
        out_specs=[near] * 2,
        scratch_shapes=[
            pltpu.VMEM((chunks, count, cb * span), tokens.dtype),
            pltpu.VMEM((rows, count), cotangent.dtype),
            pltpu.VMEM(shape, f32),
            pltpu.VMEM(shape, f32),
            pltpu.VMEM((rows_dev, topk, blocks_row), indices.dtype),
            pltpu.VMEM(wf.shape, jnp.bfloat16),
            pltpu.VMEM(wb.shape, jnp.bfloat16),
            pltpu.VMEM((chunks, n, rows_dev, cb, span), f32),
            pltpu.VMEM((chunks, n - 1, rows_dev, cb, span), f32),
            pltpu.VMEM((rows_dev * blocks_row, span), f32),
            pltpu.VMEM((reps - 1, rows_dev * blocks_row, span), f32),
            pltpu.VMEM((rows_dev * blocks_row, span), f32),
            pltpu.SemaphoreType.DMA((chunks,)),
            pltpu.SemaphoreType.DMA((6,)),
            pltpu.SemaphoreType.DMA((chunks,)),
            pltpu.SemaphoreType.DMA((chunks,)),
            pltpu.SemaphoreType.DMA((reps - 1,)),
            pltpu.SemaphoreType.DMA((reps - 1,)),
        ],
        compiler_params=pltpu.CompilerParams(
            collective_id=0, has_side_effects=True, vmem_limit_bytes=24 << 20
        ),
    )(*(pltpu.with_memory_space_constraint(x, pltpu.HBM) for x in operands))
    newp, newm = pl.pallas_call(
        put,
        out_shape=[jax.ShapeDtypeStruct(shape, f32)] * 2,
        in_specs=[near] * 2,
        out_specs=[remote] * 2,
        scratch_shapes=[pltpu.SemaphoreType.DMA((2,))],
        compiler_params=pltpu.CompilerParams(vmem_limit_bytes=1 << 20),
    )(newp, newm)
    return newp.reshape(rows_dev, width), newm.reshape(1, rows_dev, width)


def solution(mesh):
    in_specs = (
        P("rep", ("parts", "fsdp"), None),
        P("rep", ("parts", "fsdp"), None),
        P(("parts", "fsdp"), None),
        P("rep", ("parts", "fsdp"), None),
        P("rep", ("parts", "fsdp"), None, None),
    )
    out_specs = (P(("parts", "fsdp"), None), P("rep", ("parts", "fsdp"), None))
    body = functools.partial(local, mesh.shape["fsdp"], mesh.shape["rep"])
    return jax.shard_map(body, mesh=mesh, in_specs=in_specs, out_specs=out_specs, check_vma=False)
```
